32 devices in a mesh: vocab: 32 (over z, y, x, core).
Axes of the slice: x: 2, y: 2, z: 4, core: 2. Of those that a mesh axis runs over, the one named last changes fastest.
Arguments:
- hidden: bfloat16 [2, 256, 3584], P(None, 'vocab'), may hold values from -256 to 256
- head_weight: bfloat16 [3584, 24576], P(None, 'vocab'), may hold values from -1 to 1
- teacher: bfloat16 [2, 256, 24576], P(None, None, 'vocab'), may hold values from 0 to 1
Outputs:
- token_loss: float32 [2, 256], P(None, 'vocab')
- hidden_grad: bfloat16 [2, 256, 3584], P(None, 'vocab')
- head_grad: bfloat16 [3584, 24576], P(None, 'vocab')
The draws below stay inside these ranges and needn't reach their ends.
All inputs are finite; a program needn't handle non-finite values.
Results may differ from the reference program's by a relative error of at most 0.012.
Values may be sent and summed in bfloat16 or wider, within the bound.
A program may use at most 128 MiB of HBM per device.

```python
import math
import jax
import jax.numpy as jnp
from jax import lax

D = 3584
GROUP = 256
GROUPS = 2
VOCAB = 24576


def draw_head_weight(key, part):
    key_base, key_scale = jax.random.split(jax.random.fold_in(key, 11), 2)
    column_scale = jnp.exp(jax.random.uniform(key_scale, (1, VOCAB), minval=math.log(0.3), maxval=math.log(3.0)))
    base = jnp.clip(jax.random.normal(key_base, (D, VOCAB)), -6.0, 6.0)
    weight = base * column_scale / math.sqrt(D)
    return jnp.clip(weight, -1.0, 1.0).astype(jnp.bfloat16)


def draw_hidden(key, part):
    key_base, key_scale = jax.random.split(jax.random.fold_in(key, 13), 2)
    base = jnp.clip(jax.random.normal(key_base, (GROUPS, GROUP, D)), -6.0, 6.0)
    row_scale = jnp.exp(jax.random.uniform(key_scale, (GROUPS, GROUP, 1), minval=math.log(0.05), maxval=math.log(0.5)))
    states = (base * row_scale).reshape(GROUPS * GROUP, D)
    return states.reshape(GROUPS, GROUP, D).astype(jnp.bfloat16)


def draw_teacher(key, part):
    key_raw, key_weight = jax.random.split(jax.random.fold_in(key, 17), 2)
    position = jnp.arange(VOCAB, dtype=jnp.float32) / VOCAB
    raw = 2.0 * jnp.clip(jax.random.normal(key_raw, (GROUPS, GROUP, VOCAB)), -6.0, 6.0)
    log_mean = 2.0
    rising = math.log(3.0)
    shift_value = log_mean + math.log(VOCAB) + math.log((math.exp(rising) - 1.0) / rising)
    token_weight = jax.random.uniform(key_weight, (GROUPS, GROUP, 1), minval=0.5, maxval=1.5)
    probable = token_weight * jnp.exp(raw + rising * position - shift_value)
    return jnp.clip(probable, 0.0, 1.0).astype(jnp.bfloat16)


def setup_inputs(seed: int = 0) -> dict:
    splits = jax.random.split(jax.random.key(seed), 4)
    hidden = draw_hidden(jax.random.fold_in(splits[3], 71), 0)
    head_weight = draw_head_weight(jax.random.fold_in(splits[3], 71), 0)
    teacher = draw_teacher(jax.random.fold_in(splits[3], 71), 0)
    return {"hidden": hidden, "head_weight": head_weight, "teacher": teacher}


def reference(hidden, head_weight, teacher):
    loss_list = []
    hidden_list = []
    weight_grad = jnp.zeros(head_weight.shape, jnp.bfloat16)
    for group_index in range(GROUPS):
        logit_block = jnp.dot(hidden[group_index], head_weight, preferred_element_type=jnp.float32)
        target_wide = teacher[group_index].astype(jnp.float32)
        peak_logit = jnp.max(logit_block, axis=-1, keepdims=True)
        exp_total = jnp.sum(jnp.exp(logit_block - peak_logit), axis=-1, keepdims=True)
        log_norm = peak_logit + jnp.log(exp_total)
        teacher_mass = jnp.sum(target_wide, axis=-1, keepdims=True)
        cross_term = jnp.sum(target_wide * logit_block, axis=-1, keepdims=True)
        loss_list.append((teacher_mass * log_norm - cross_term)[:, 0])
        logit_grad = (teacher_mass * jnp.exp(logit_block - log_norm) - target_wide).astype(jnp.bfloat16)
        hidden_list.append(jnp.dot(logit_grad, head_weight.T, preferred_element_type=jnp.float32).astype(jnp.bfloat16))
        product_term = lax.dot_general(hidden[group_index], logit_grad, (((0,), (0,)), ((), ())), preferred_element_type=jnp.float32)
        weight_grad = (weight_grad.astype(jnp.float32) + product_term).astype(jnp.bfloat16)
    return (jnp.stack(loss_list), jnp.stack(hidden_list), weight_grad)
```

```python
import jax
import jax.numpy as jnp
from jax import lax
from jax.experimental import pallas as pl
from jax.experimental.pallas import tpu as pltpu
from jax.sharding import PartitionSpec as P
import functools

MESH = pl.DeviceIdType.MESH


def finish(logit_block, target_block):
    target_wide = target_block.astype(jnp.float32)
    teacher_mass = jnp.sum(target_wide, axis=-1)
    cross_term = jnp.sum(target_wide * logit_block, axis=-1)
    peak_logit = jnp.max(logit_block, axis=-1)
    peak_logit = lax.pmax(peak_logit, "vocab")
    exp_total = jnp.sum(jnp.exp(logit_block - peak_logit[..., None]), axis=-1)
    exp_total, teacher_mass, cross_term = lax.psum((exp_total, teacher_mass, cross_term), "vocab")
    log_norm = peak_logit + jnp.log(exp_total)
    token_loss = teacher_mass * log_norm - cross_term
    logit_grad = (
        teacher_mass[..., None] * jnp.exp(logit_block - log_norm[..., None]) - target_wide
    ).astype(jnp.bfloat16)
    return (token_loss, logit_grad)


def plain_shards(hidden, head_weight, teacher):
    group_count, row_count, model_width = hidden.shape
    contract = (((1,), (1,)), ((), ()))
    shard_rows = lax.all_gather(hidden, "vocab", axis=1, tiled=True)
    logits = jnp.einsum("crd,dv->crv", shard_rows, head_weight, preferred_element_type=jnp.float32)
    token_loss, logit_grad = finish(logits, teacher)
    row_total = lax.axis_size("vocab") * (group_count * row_count)
    per_group = row_total // group_count
    owner_count = per_group // row_count
    grad_block = logit_grad
    grad_block = (
        grad_block.reshape(group_count, owner_count, row_count, -1)
        .transpose(1, 0, 2, 3)
        .reshape(row_total, -1)
    )
    summed = lax.psum_scatter(
        lax.dot_general(grad_block, head_weight, contract, preferred_element_type=jnp.float32),
        "vocab",
        scatter_dimension=0,
        tiled=True,
    )
    hidden_grad = summed.reshape(group_count, row_count, model_width).astype(jnp.bfloat16)
    weight_grad = jnp.zeros((model_width, head_weight.shape[1]), jnp.bfloat16)
    for group_index in range(group_count):
        product_term = lax.dot_general(
            shard_rows[group_index],
            logit_grad[group_index],
            (((0,), (0,)), ((), ())),
            preferred_element_type=jnp.float32,
        )
        weight_grad = (weight_grad.astype(jnp.float32) + product_term).astype(jnp.bfloat16)
    own_loss = lax.dynamic_slice_in_dim(
        token_loss, lax.axis_index("vocab") * row_count, row_count, 1
    )
    return (own_loss, hidden_grad, weight_grad)


def subsets(bits):
    masks = [0]
    for b in bits:
        masks += [m | (1 << b) for m in masks]
    return masks


def axis_orders(bit_count):
    axes = [[b] for b in range(1, min(bit_count, 3))] + [list(range(bit_count - 1, 2, -1))]
    x, y, z = axes
    return [z + y + x + [0], y + x + z + [0], x + z + y + [0]]


def kernel(n, parts, hid, w_hbm, t_hbm, hfull, dl_hbm, hgrad, loss,
           hbuf, w, t, logits, dl, g, rbuf, st, stc, wide,
           ag_send, ag_recv, rs_send, rs_recv, st_send, st_recv, local):
    bit_count = n.bit_length() - 1
    me = lax.axis_index("vocab")
    flip = [(1 - 2 * ((me // (1 << b)) % 2)) * (1 << b) for b in range(bit_count)]

    def at(mask):
        return me + sum(flip[b] for b in range(bit_count) if mask >> b & 1)

    rows, width = hid.shape
    tokens, columns = dl.shape
    orders = axis_orders(bit_count)
    part_ids = range(len(parts))

    copy_w = [
        pltpu.make_async_copy(w_hbm.at[pl.ds(o, c)], w.at[pl.ds(o, c)], local.at[i])
        for i, (o, c) in enumerate(parts)
    ]
    copy_t = pltpu.make_async_copy(t_hbm, t, local.at[3])
    copy_own = pltpu.make_async_copy(hid, hbuf.at[me], local.at[4])
    copy_own.start()

    barrier = pltpu.get_barrier_semaphore()
    for b in range(bit_count):
        pl.semaphore_signal(barrier, inc=1, device_id=(at(1 << b),), device_id_type=MESH)
    pl.semaphore_wait(barrier, bit_count)
    copy_own.wait()

    def gather_copy(p, b, r):
        o, c = parts[p]
        block = hbuf.at[at(r), :, pl.ds(o, c)]
        k = r | (1 << b)
        return pltpu.make_async_remote_copy(
            src_ref=block, dst_ref=block,
            send_sem=ag_send.at[p, k], recv_sem=ag_recv.at[p, k],
            device_id=(at(1 << b),), device_id_type=MESH)

    def gather_arrival(p, b, r):
        o, c = parts[p]
        block = hbuf.at[at(r | (1 << b)), :, pl.ds(o, c)]
        k = r | (1 << b)
        return pltpu.make_async_remote_copy(
            src_ref=block, dst_ref=block,
            send_sem=ag_send.at[p, k], recv_sem=ag_recv.at[p, k],
            device_id=(at(1 << b),), device_id_type=MESH)

    def logits_part(p):
        o, c = parts[p]
        copy_w[p].wait()

        @pl.loop(0, columns // 256)
        def _(j):
            cols = pl.ds(pl.multiple_of(j * 256, 256), 256)
            term = jnp.dot(hbuf[:, :, o:o + c].reshape(tokens, c), w[o:o + c, cols],
                           preferred_element_type=jnp.float32)
            if p == 0:
                logits[:, cols] = term
            else:
                logits[:, cols] += term

    for s in range(bit_count):
        for p in part_ids:
            b = orders[p][s]
            if s:
                prev = orders[p][s - 1]
                for r in subsets(orders[p][:s - 1]):
                    gather_arrival(p, prev, r).wait_recv()
            for r in subsets(orders[p][:s]):
                gather_copy(p, b, r).start()
        if s == 0:
            for p in part_ids:
                copy_w[p].start()
            copy_t.start()
    for p in part_ids:
        for r in subsets(orders[p][:-1]):
            gather_arrival(p, orders[p][-1], r).wait_recv()
        logits_part(p)
    for p in part_ids:
        for s in range(bit_count):
            for r in subsets(orders[p][:s]):
                gather_copy(p, orders[p][s], r).wait_send()
    out_h = pltpu.make_async_copy(hbuf, hfull, local.at[5])
    out_h.start()
    copy_t.wait()

    chunk = 64

    @pl.loop(0, tokens // chunk)
    def _(i):
        ds = pl.ds(pl.multiple_of(i * chunk, chunk), chunk)
        l = logits[ds, :]
        tw = t[ds, :].astype(jnp.float32)
        peak = jnp.max(l, axis=-1, keepdims=True)
        total = jnp.sum(jnp.exp(l - peak), axis=-1, keepdims=True)
        mass = jnp.sum(tw, axis=-1, keepdims=True)
        cross = jnp.sum(tw * l, axis=-1, keepdims=True)
        lane = lax.broadcasted_iota(jnp.int32, (chunk, 128), 1)
        st[ds, :] = jnp.where(lane == 0, peak, jnp.where(lane == 1, total, jnp.where(lane == 2, mass, cross)))

    stc[0] = st[...].T[0:8]
    for b in range(bit_count):
        copy = pltpu.make_async_remote_copy(
            src_ref=stc.at[2 * b], dst_ref=stc.at[2 * b + 1],
            send_sem=st_send.at[b], recv_sem=st_recv.at[b],
            device_id=(at(1 << b),), device_id_type=MESH)
        copy.start()
        copy.wait()
        mine, other = stc[2 * b], stc[2 * b + 1]
        peak = jnp.maximum(mine[0:1], other[0:1])
        total = mine[1:2] * jnp.exp(mine[0:1] - peak) + other[1:2] * jnp.exp(other[0:1] - peak)
        sums = mine + other
        row = lax.broadcasted_iota(jnp.int32, sums.shape, 0)
        stc[2 * b + 2] = jnp.where(row == 0, peak, jnp.where(row == 1, total, sums))
    final = stc[2 * bit_count]
    log_norm = final[0:1] + jnp.log(final[1:2])
    mass = final[2:3]
    loss[...] = jnp.broadcast_to(mass * log_norm - final[3:4], loss.shape)
    row = lax.broadcasted_iota(jnp.int32, (8, tokens), 0)
    wide[...] = jnp.zeros(wide.shape, jnp.float32)
    wide[0:8] = jnp.where(row == 0, log_norm, mass)
    st[...] = wide[...].T

    @pl.loop(0, tokens // chunk)
    def _(i):
        ds = pl.ds(pl.multiple_of(i * chunk, chunk), chunk)
        s = st[ds, :]
        dl[ds, :] = (s[:, 1:2] * jnp.exp(logits[ds, :] - s[:, 0:1]) - t[ds, :].astype(jnp.float32)).astype(jnp.bfloat16)

    out_dl = pltpu.make_async_copy(dl, dl_hbm, local.at[6])
    out_dl.start()

    def scatter_copy(p, s, r):
        o, c = parts[p]
        b = orders[p][bit_count - 1 - s]
        k = r | (1 << b)
        return pltpu.make_async_remote_copy(
            src_ref=g.at[at(k), :, pl.ds(o, c)], dst_ref=rbuf.at[k, :, pl.ds(o, c)],
            send_sem=rs_send.at[p, k], recv_sem=rs_recv.at[p, k],
            device_id=(at(1 << b),), device_id_type=MESH)

    def left(p, s):
        return subsets(orders[p][:bit_count - 1 - s])

    for p in part_ids:
        o, c = parts[p]

        @pl.loop(0, c // 256)
        def _(j):
            ds = pl.ds(pl.multiple_of(o + j * 256, 256), 256)
            term = lax.dot_general(dl[...], w[ds, :], (((1,), (1,)), ((), ())),
                                   preferred_element_type=jnp.float32)
            g[:, :, ds] = term.astype(jnp.bfloat16).reshape(n, rows, 256)

        for r in left(p, 0):
            scatter_copy(p, 0, r).start()
    for s in range(bit_count):
        for p in part_ids:
            o, c = parts[p]
            b = orders[p][bit_count - 1 - s]
            for r in left(p, s):
                scatter_copy(p, s, r).wait_recv()
                k = r | (1 << b)
                total = g[at(r), :, o:o + c].astype(jnp.float32) + rbuf[k, :, o:o + c].astype(jnp.float32)
                if s == bit_count - 1:
                    hgrad[:, o:o + c] = total.astype(jnp.bfloat16)
                else:
                    g[at(r), :, o:o + c] = total.astype(jnp.bfloat16)
            if s < bit_count - 1:
                for r in left(p, s + 1):
                    scatter_copy(p, s + 1, r).start()
    for p in part_ids:
        for s in range(bit_count):
            for r in left(p, s):
                scatter_copy(p, s, r).wait_send()
    out_h.wait()
    out_dl.wait()


def split_width(width):
    tiles = width // 256
    third = -(-tiles // 3)
    sizes = [third, tiles - 2 * third, third]
    parts, at = [], 0
    for size in sizes:
        parts.append((at * 256, size * 256))
        at += size
    return parts


def shards(n, hidden, head_weight, teacher):
    group_count, row_count, width = hidden.shape
    columns = head_weight.shape[1]
    rows = group_count * row_count
    tokens = n * rows
    bf16, f32 = jnp.bfloat16, jnp.float32
    bit_count = n.bit_length() - 1
    parts = split_width(width)
    by_owner = (
        teacher.reshape(group_count, n, row_count, columns).transpose(1, 0, 2, 3).reshape(tokens, columns)
    )
    vmem = pl.BlockSpec(memory_space=pltpu.VMEM)
    hbm = pl.BlockSpec(memory_space=pl.ANY)
    dma = pltpu.SemaphoreType.DMA
    hfull, dl, hgrad, loss = pl.pallas_call(
        functools.partial(kernel, n, parts),
        out_shape=[
            jax.ShapeDtypeStruct((n, rows, width), bf16),
            jax.ShapeDtypeStruct((tokens, columns), bf16),
            jax.ShapeDtypeStruct((rows, width), bf16),
            jax.ShapeDtypeStruct((8, tokens), f32),
        ],
        in_specs=[vmem, hbm, hbm],
        out_specs=[hbm, hbm, vmem, vmem],
        scratch_shapes=[
            pltpu.VMEM((n, rows, width), bf16),
            pltpu.VMEM((width, columns), bf16),
            pltpu.VMEM((tokens, columns), bf16),
            pltpu.VMEM((tokens, columns), f32),
            pltpu.VMEM((tokens, columns), bf16),
            pltpu.VMEM((n, rows, width), bf16),
            pltpu.VMEM((n, rows, width), bf16),
            pltpu.VMEM((tokens, 128), f32),
            pltpu.VMEM((2 * bit_count + 1, 8, tokens), f32),
            pltpu.VMEM((128, tokens), f32),
            dma((3, n)), dma((3, n)), dma((3, n)), dma((3, n)),
            dma((bit_count,)), dma((bit_count,)), dma((8,)),
        ],
        compiler_params=pltpu.CompilerParams(
            collective_id=0, has_side_effects=True, vmem_limit_bytes=58 * 1024 * 1024),
    )(hidden.reshape(rows, width), head_weight, by_owner)
    weight_grad = lax.dot_general(
        hfull.reshape(tokens, width), dl, (((0,), (0,)), ((), ())), preferred_element_type=f32
    ).astype(bf16)
    own_loss = lax.dynamic_slice_in_dim(loss[0], lax.axis_index("vocab") * rows, rows, 0)
    return (own_loss.reshape(group_count, row_count), hgrad.reshape(group_count, row_count, width), weight_grad)


def choose(n, hidden, head_weight, teacher):
    group_count, row_count, width = hidden.shape
    fits = (
        n >= 16 and n & (n - 1) == 0 and group_count * row_count % 16 == 0
        and width % 256 == 0 and width >= 1024 and head_weight.shape[1] % 256 == 0
    )
    if fits:
        return shards(n, hidden, head_weight, teacher)
    return plain_shards(hidden, head_weight, teacher)


def solution(mesh):
    in_specs = (P(None, "vocab", None), P(None, "vocab"), P(None, None, "vocab"))
    out_specs = (P(None, "vocab"), P(None, "vocab", None), P(None, "vocab"))
    return jax.shard_map(functools.partial(choose, mesh.shape["vocab"]), mesh=mesh, in_specs=in_specs, out_specs=out_specs, check_vma=False)
```

```python
import jax
import jax.numpy as jnp
from jax import lax
from jax.experimental import pallas as pl
from jax.experimental.pallas import tpu as pltpu
from jax.sharding import PartitionSpec as P
import functools

MESH = pl.DeviceIdType.MESH


def finish(logit_block, target_block):
    target_wide = target_block.astype(jnp.float32)
    teacher_mass = jnp.sum(target_wide, axis=-1)
    cross_term = jnp.sum(target_wide * logit_block, axis=-1)
    peak_logit = jnp.max(logit_block, axis=-1)
    peak_logit = lax.pmax(peak_logit, "vocab")
    exp_total = jnp.sum(jnp.exp(logit_block - peak_logit[..., None]), axis=-1)
    exp_total, teacher_mass, cross_term = lax.psum((exp_total, teacher_mass, cross_term), "vocab")
    log_norm = peak_logit + jnp.log(exp_total)
    token_loss = teacher_mass * log_norm - cross_term
    logit_grad = (
        teacher_mass[..., None] * jnp.exp(logit_block - log_norm[..., None]) - target_wide
    ).astype(jnp.bfloat16)
    return (token_loss, logit_grad)


def plain_shards(hidden, head_weight, teacher):
    group_count, row_count, model_width = hidden.shape
    contract = (((1,), (1,)), ((), ()))
    shard_rows = lax.all_gather(hidden, "vocab", axis=1, tiled=True)
    logits = jnp.einsum("crd,dv->crv", shard_rows, head_weight, preferred_element_type=jnp.float32)
    token_loss, logit_grad = finish(logits, teacher)
    row_total = lax.axis_size("vocab") * (group_count * row_count)
    per_group = row_total // group_count
    owner_count = per_group // row_count
    grad_block = logit_grad
    grad_block = (
        grad_block.reshape(group_count, owner_count, row_count, -1)
        .transpose(1, 0, 2, 3)
        .reshape(row_total, -1)
    )
    summed = lax.psum_scatter(
        lax.dot_general(grad_block, head_weight, contract, preferred_element_type=jnp.float32),
        "vocab",
        scatter_dimension=0,
        tiled=True,
    )
    hidden_grad = summed.reshape(group_count, row_count, model_width).astype(jnp.bfloat16)
    weight_grad = jnp.zeros((model_width, head_weight.shape[1]), jnp.bfloat16)
    for group_index in range(group_count):
        product_term = lax.dot_general(
            shard_rows[group_index],
            logit_grad[group_index],
            (((0,), (0,)), ((), ())),
            preferred_element_type=jnp.float32,
        )
        weight_grad = (weight_grad.astype(jnp.float32) + product_term).astype(jnp.bfloat16)
    own_loss = lax.dynamic_slice_in_dim(
        token_loss, lax.axis_index("vocab") * row_count, row_count, 1
    )
    return (own_loss, hidden_grad, weight_grad)


def subsets(masks):
    out = [0]
    for m in masks:
        out += [o ^ m for o in out]
    return out


def axis_orders(n):
    z = [1 << b for b in range(n.bit_length() - 2, 2, -1)]
    return {"zyx": z + [4, 2, 1], "xzy": [2] + z + [4, 1], "yxz": [4, 2] + z + [1]}


def kernel(n, parts, groups, hid, w_hbm, t_hbm, hfull, dl_hbm, hgrad, loss,
           hbuf, w, t, logits, dl, g, rbuf, st, stc,
           ag_send, ag_recv, rs_send, rs_recv, st_send, st_recv, local):
    bit_count = n.bit_length() - 1
    me = lax.axis_index("vocab")
    flip = [(1 - 2 * ((me // (1 << b)) % 2)) * (1 << b) for b in range(bit_count)]

    def at(mask):
        return me + sum(flip[b] for b in range(bit_count) if mask >> b & 1)

    rows, width = hid.shape
    tokens, columns = dl.shape
    part_ids = range(len(parts))
    orders = [order for _, _, order in parts]
    near = subsets([1, 2, 4])[1:]
    far = subsets([1 << b for b in range(3, bit_count)])[1:]
    peers = sorted(set(near + far + [m for order in orders for m in order]))

    copy_w = [
        pltpu.make_async_copy(w_hbm.at[pl.ds(o, c)], w.at[pl.ds(o, c)], local.at[i])
        for i, (o, c, _) in enumerate(parts)
    ]
    base = len(parts)
    copy_t = [
        pltpu.make_async_copy(t_hbm.at[c], t.at[:, c], local.at[base + 3 + c]) for c in range(groups)
    ]
    copy_own = pltpu.make_async_copy(hid, hbuf.at[me], local.at[base])
    copy_own.start()

    barrier = pltpu.get_barrier_semaphore()
    for mask in peers:
        pl.semaphore_signal(barrier, inc=1, device_id=(at(mask),), device_id_type=MESH)
    pl.semaphore_wait(barrier, len(peers))
    copy_own.wait()

    def gather_copy(p, b, r):
        o, c, _ = parts[p]
        block = hbuf.at[at(r), :, pl.ds(o, c)]
        return pltpu.make_async_remote_copy(
            src_ref=block, dst_ref=block,
            send_sem=ag_send.at[p, r ^ b], recv_sem=ag_recv.at[p, r ^ b],
            device_id=(at(b),), device_id_type=MESH)

    def gather_arrival(p, b, r):
        o, c, _ = parts[p]
        block = hbuf.at[at(r ^ b), :, pl.ds(o, c)]
        return pltpu.make_async_remote_copy(
            src_ref=block, dst_ref=block,
            send_sem=ag_send.at[p, r ^ b], recv_sem=ag_recv.at[p, r ^ b],
            device_id=(at(b),), device_id_type=MESH)

    def logits_part(p):
        o, c, _ = parts[p]
        copy_w[p].wait()

        @pl.loop(0, columns // 256)
        def _(j):
            cols = pl.ds(pl.multiple_of(j * 256, 256), 256)
            term = jnp.dot(hbuf[:, :, o:o + c].reshape(tokens, c), w[o:o + c, cols],
                           preferred_element_type=jnp.float32)
            if p == 0:
                logits[:, cols] = term
            else:
                logits[:, cols] += term

    for s in range(bit_count):
        for p in part_ids:
            gather_copy(p, orders[p][s], 0).start()
    for p in part_ids:
        copy_w[p].start()
    for copy in copy_t:
        copy.start()
    for s in range(bit_count - 1):
        for p in part_ids:
            b = orders[p][s]
            for r in subsets(orders[p][:s]):
                gather_arrival(p, b, r).wait_recv()
                for later in orders[p][s + 1:]:
                    gather_copy(p, later, r ^ b).start()
    for p in part_ids:
        for r in subsets(orders[p][:-1]):
            gather_arrival(p, orders[p][-1], r).wait_recv()
        logits_part(p)
    out_h = pltpu.make_async_copy(hbuf, hfull, local.at[base + 1])
    out_h.start()
    for copy in copy_t:
        copy.wait()

    chunk = 64
    owners = chunk // rows

    def teacher_rows(i):
        part = t[pl.ds(i * owners, owners)]
        return part.astype(jnp.float32).reshape(chunk, columns)

    @pl.loop(0, tokens // chunk)
    def _(i):
        ds = pl.ds(pl.multiple_of(i * chunk, chunk), chunk)
        l = logits[ds, :]
        tw = teacher_rows(i)
        peak = jnp.max(l, axis=-1, keepdims=True)
        total = jnp.sum(jnp.exp(l - peak), axis=-1, keepdims=True)
        mass = jnp.sum(tw, axis=-1, keepdims=True)
        cross = jnp.sum(tw * l, axis=-1, keepdims=True)
        lane = lax.broadcasted_iota(jnp.int32, (chunk, 128), 1)
        st[ds, :] = jnp.where(lane == 0, peak, jnp.where(lane == 1, total, jnp.where(lane == 2, mass, cross)))

    lines = tokens // 128
    for j in range(lines):
        turned = st[j * 128:(j + 1) * 128, :].T
        for k in range(4):
            stc[0, k, j:j + 1, :] = turned[k:k + 1]

    def exchange(source, masks):
        copies = [
            pltpu.make_async_remote_copy(
                src_ref=stc.at[source], dst_ref=stc.at[mask],
                send_sem=st_send.at[mask], recv_sem=st_recv.at[mask],
                device_id=(at(mask),), device_id_type=MESH)
            for mask in masks
        ]
        for copy in copies:
            copy.start()
        for copy in copies:
            copy.wait()
        slots = [source] + masks
        peak = functools.reduce(jnp.maximum, [stc[m, 0] for m in slots])
        total = sum(stc[m, 1] * jnp.exp(stc[m, 0] - peak) for m in slots)
        return peak, total, sum(stc[m, 2] for m in slots), sum(stc[m, 3] for m in slots)

    for k, value in enumerate(exchange(0, near)):
        stc[n, k] = value
    peak, total, mass, cross = exchange(n, far)
    log_norm = peak + jnp.log(total)
    line = lax.broadcasted_iota(jnp.int32, (128, 128), 0)
    for j in range(lines):
        st[j * 128:(j + 1) * 128, :] = jnp.where(line == 0, log_norm[j:j + 1], mass[j:j + 1]).T

    @pl.loop(0, tokens // chunk)
    def _(i):
        ds = pl.ds(pl.multiple_of(i * chunk, chunk), chunk)
        s = st[ds, :]
        dl[ds, :] = (s[:, 1:2] * jnp.exp(logits[ds, :] - s[:, 0:1]) - teacher_rows(i)).astype(jnp.bfloat16)

    out_dl = pltpu.make_async_copy(dl, dl_hbm, local.at[base + 2])
    out_dl.start()

    def scatter_copy(p, b, k):
        o, c, _ = parts[p]
        return pltpu.make_async_remote_copy(
            src_ref=g.at[at(k), :, pl.ds(o, c)], dst_ref=rbuf.at[k, :, pl.ds(o, c)],
            send_sem=rs_send.at[p, k], recv_sem=rs_recv.at[p, k],
            device_id=(at(b),), device_id_type=MESH)

    backs = [order[::-1] for order in orders]

    for p in part_ids:
        o, c, _ = parts[p]

        @pl.loop(0, c // 256)
        def _(j):
            ds = pl.ds(pl.multiple_of(o + j * 256, 256), 256)
            term = lax.dot_general(dl[...], w[ds, :], (((1,), (1,)), ((), ())),
                                   preferred_element_type=jnp.float32)
            g[:, :, ds] = term.astype(jnp.bfloat16).reshape(n, rows, 256)

        for r in subsets(backs[p][:0:-1])[::-1]:
            scatter_copy(p, backs[p][0], r ^ backs[p][0]).start()

    def reduced(p, s, k):
        o, c, _ = parts[p]
        total = g[at(k), :, o:o + c].astype(jnp.float32)
        for b in backs[p][:s]:
            scatter_copy(p, b, k ^ b).wait_recv()
            total += rbuf[k ^ b, :, o:o + c].astype(jnp.float32)
        return total.astype(jnp.bfloat16)

    for s in range(1, bit_count):
        for p in part_ids:
            o, c, _ = parts[p]
            b = backs[p][s]
            for r in subsets(backs[p][:s:-1])[::-1]:
                g[at(r ^ b), :, o:o + c] = reduced(p, s, r ^ b)
                scatter_copy(p, b, r ^ b).start()
    for p in part_ids:
        o, c, _ = parts[p]
        hgrad[:, o:o + c] = reduced(p, bit_count, 0)

    group_rows = rows // groups
    value = mass * log_norm - cross
    token = lax.broadcasted_iota(jnp.int32, value.shape, 0) * 128 + lax.broadcasted_iota(jnp.int32, value.shape, 1)
    first = me * rows
    picked = []
    for c in range(groups):
        start = first + c * group_rows
        own = jnp.where((token >= start) & (token < start + group_rows), value, 0.0)
        picked.append(jnp.sum(own, axis=0, keepdims=True))
    spread = (
        lax.broadcasted_iota(jnp.int32, (128, group_rows), 0) % group_rows
        == lax.broadcasted_iota(jnp.int32, (128, group_rows), 1)
    ).astype(jnp.float32)
    loss[...] = jnp.dot(jnp.concatenate(picked, axis=0), spread, precision=lax.Precision.HIGHEST,
                        preferred_element_type=jnp.float32)

    for p in part_ids:
        for s in range(bit_count):
            for r in subsets(orders[p][:s]):
                gather_copy(p, orders[p][s], r).wait_send()
            for r in subsets(backs[p][s + 1:]):
                scatter_copy(p, backs[p][s], r ^ backs[p][s]).wait_send()
    out_h.wait()
    out_dl.wait()


def split_width(width, orders):
    tiles = width // 256
    last = max(1, tiles // 14)
    second = max(1, tiles * 5 // 14)
    first = tiles - second - last
    half = first // 2
    sizes = [(half, "zyx"), (second, "xzy"), (first - half, "zyx"), (last, "yxz")]
    parts, at = [], 0
    for size, name in sizes:
        if size:
            parts.append((at * 256, size * 256, orders[name]))
            at += size
    return parts


def shards(n, hidden, head_weight, teacher):
    group_count, row_count, width = hidden.shape
    columns = head_weight.shape[1]
    rows = group_count * row_count
    tokens = n * rows
    bf16, f32 = jnp.bfloat16, jnp.float32
    parts = split_width(width, axis_orders(n))
    count = len(parts)
    vmem = pl.BlockSpec(memory_space=pltpu.VMEM)
    hbm = pl.BlockSpec(memory_space=pl.ANY)
    dma = pltpu.SemaphoreType.DMA
    hfull, dl, hgrad, loss = pl.pallas_call(
        functools.partial(kernel, n, parts, group_count),
        out_shape=[
            jax.ShapeDtypeStruct((n, rows, width), bf16),
            jax.ShapeDtypeStruct((tokens, columns), bf16),
            jax.ShapeDtypeStruct((rows, width), bf16),
            jax.ShapeDtypeStruct((group_count, row_count), f32),
        ],
        in_specs=[vmem, hbm, hbm],
        out_specs=[hbm, hbm, vmem, vmem],
        scratch_shapes=[
            pltpu.VMEM((n, rows, width), bf16),
            pltpu.VMEM((width, columns), bf16),
            pltpu.VMEM((n, group_count, row_count, columns), bf16),
            pltpu.VMEM((tokens, columns), f32),
            pltpu.VMEM((tokens, columns), bf16),
            pltpu.VMEM((n, rows, width), bf16),
            pltpu.VMEM((n, rows, width), bf16),
            pltpu.VMEM((tokens, 128), f32),
            pltpu.VMEM((n + 1, 4, tokens // 128, 128), f32),
            dma((count, n)), dma((count, n)), dma((count, n)), dma((count, n)),
            dma((n,)), dma((n,)), dma((count + 3 + group_count,)),
        ],
        compiler_params=pltpu.CompilerParams(
            collective_id=0, has_side_effects=True, vmem_limit_bytes=58 * 1024 * 1024),
    )(hidden.reshape(rows, width), head_weight, teacher.reshape(group_count, n, row_count, columns))
    weight_grad = lax.dot_general(
        hfull.reshape(tokens, width), dl, (((0,), (0,)), ((), ())), preferred_element_type=f32
    ).astype(bf16)
    return (loss, hgrad.reshape(group_count, row_count, width), weight_grad)


def choose(n, hidden, head_weight, teacher):
    group_count, row_count, width = hidden.shape
    fits = (
        n >= 16 and n & (n - 1) == 0 and group_count * row_count in (16, 32, 64) and row_count % 8 == 0
        and n * group_count * row_count % 128 == 0 and 128 % row_count == 0
        and width % 256 == 0 and width >= 1024 and head_weight.shape[1] % 256 == 0
    )
    if fits:
        return shards(n, hidden, head_weight, teacher)
    return plain_shards(hidden, head_weight, teacher)


def solution(mesh):
    in_specs = (P(None, "vocab", None), P(None, "vocab"), P(None, None, "vocab"))
    out_specs = (P(None, "vocab"), P(None, "vocab", None), P(None, "vocab"))
    return jax.shard_map(functools.partial(choose, mesh.shape["vocab"]), mesh=mesh, in_specs=in_specs, out_specs=out_specs, check_vma=False)
```
